32 devices in a mesh: chain: 8 (over z, x), col: 4 (over y, core).
Axes of the slice: x: 2, y: 2, z: 4, core: 2. Of those that a mesh axis runs over, the one named last changes fastest.
Arguments:
- inverses: float32 [8, 2, 512, 512], P('chain', None, None, 'col'), may hold values from -3 to 3
- couplings: float32 [8, 2, 512, 512], P('chain', None, None, 'col'), may hold values from -3 to 3
- sources: float32 [8, 2, 512, 1024], P('chain', None, None, 'col'), may hold values from -6 to 6
- counts: int32 [8], P('chain'), may hold values from 384 to 512, as said below
Outputs:
- fields: float32 [8, 2, 512, 1024], P('chain', None, None, 'col')
The draws below stay inside these ranges and needn't reach their ends.
Inputs may be any that keep to these rules, and one draw needn't show every extreme that they name: `counts`: some slice has exactly 512 orbitals in use.
All inputs are finite; a program needn't handle non-finite values.
Results may differ from the reference program's by a relative error of at most 0.0003.
Values sent between devices are 32-bit elements; how exact they have to be, the bound alone decides.
No kernel may reach another device: no remote copies, remote signals or barrier semaphores. Data moves between devices by JAX's collectives and lax.ppermute only.
A program may use at most 128 MiB of HBM per device.

```python
import math
import jax
import jax.numpy as jnp
from jax import lax

B = 512
SLICE_COUNT = 8
R = 1024


def rate_table(key):
    root_random_key = jax.random.fold_in(key, 7)
    category_key, quick_rate_key, spike_key, amplification_key = jax.random.split(root_random_key, 4)
    slow_share = 0.5
    sluggish_mask = jax.random.uniform(category_key, (B,)) < slow_share
    fast_rates = jax.random.uniform(quick_rate_key, (B,), minval=0.9, maxval=0.95)
    conduction_channel_rates = jnp.where(sluggish_mask, 0.975, fast_rates)
    spike_mask = jax.random.randint(spike_key, (SLICE_COUNT, 1), 0, 12) == 0
    spike_multiplier = jnp.where(spike_mask & sluggish_mask[None, :], 0.6, 1.0)
    per_slice_rates = conduction_channel_rates[None, :] * spike_multiplier
    slice_gains = jnp.exp(jax.random.uniform(amplification_key, (SLICE_COUNT, B), minval=-0.35, maxval=0.35))
    return (per_slice_rates, slice_gains)


def noisy_blocks(key, diagonal_values):
    noise_draw = jnp.clip(jax.random.normal(key, (SLICE_COUNT, 2, B, B)), -6.0, 6.0) * (0.08 / math.sqrt(B))
    identity_matrix = jnp.eye(B, dtype=jnp.float32)
    real_part = noise_draw[:, 0] + diagonal_values[:, :, None] * identity_matrix[None, :, :]
    return jnp.stack([real_part, noise_draw[:, 1]], axis=1).astype(jnp.float32)


def draw_inverses(key, part):
    per_slice_rates, slice_gains = rate_table(key)
    return noisy_blocks(jax.random.fold_in(key, 21), slice_gains)


def draw_couplings(key, part):
    per_slice_rates, slice_gains = rate_table(key)
    return noisy_blocks(jax.random.fold_in(key, 22), per_slice_rates / slice_gains)


def draw_counts(key, part):
    count_key = jax.random.fold_in(key, 5)
    drawn = jax.random.randint(count_key, (SLICE_COUNT,), 3 * B // 4, B + 1)
    chosen_slice = jax.random.randint(jax.random.fold_in(count_key, 1), (), 0, SLICE_COUNT)
    return jnp.where(jnp.arange(SLICE_COUNT) == chosen_slice, B, drawn).astype(jnp.int32)


def block_scale(key, dims, pieces, least, largest):
    loudness, own = 1.0, jax.random.fold_in(key, 6)
    for position, blocks in pieces:
        steps = jnp.exp(jax.random.uniform(jax.random.fold_in(own, position), (blocks,), jnp.float32, least / len(pieces), largest / len(pieces)))
        loudness = loudness * jnp.repeat(steps, dims[position] // blocks).reshape([-1 if axis == position else 1 for axis in range(len(dims))])
    return loudness


def centred(stream_key, shape, scale, bound, pieces=(), held_as=jnp.bfloat16):
    entries = jax.random.normal(stream_key, shape, jnp.float32) * scale
    if len(pieces) > 0:
        entries = block_scale(stream_key, shape, pieces, -0.22, 0.18) * entries
    return jnp.clip(entries, min=-bound, max=bound).astype(held_as)


def setup_inputs(seed: int = 0) -> dict:
    key_of = jax.random.split(jax.random.key(seed), 5)
    inverses = draw_inverses(jax.random.fold_in(key_of[4], 71), 0)
    couplings = draw_couplings(jax.random.fold_in(key_of[4], 71), 0)
    sources = centred(key_of[2], (SLICE_COUNT, 2, B, R), 1.0, 6.0, ((0, 8), (3, 4)), jnp.float32)
    counts = draw_counts(jax.random.fold_in(key_of[4], 71), 0)
    return dict(inverses=inverses, couplings=couplings, sources=sources, counts=counts)


def real_product(left_side, right_side):
    return jnp.dot(left_side, right_side, precision=lax.Precision.HIGHEST, preferred_element_type=jnp.float32)


def complex_product(left_side, right_side):
    real_part = real_product(left_side[0], right_side[0]) - real_product(left_side[1], right_side[1])
    imag_part = real_product(left_side[0], right_side[1]) + real_product(left_side[1], right_side[0])
    return jnp.stack([real_part, imag_part])


def reference(inverses, couplings, sources, counts):
    row_index = lax.iota(jnp.int32, B)

    def advance(carried_state, slice_items):
        inverse_block, coupling_block, source_block, active_count = slice_items
        active = (row_index < active_count).astype(jnp.float32)[:, None]
        updated = active * complex_product(inverse_block, source_block + complex_product(coupling_block, carried_state))
        return updated, updated

    zero_state = jnp.zeros((2, B, R), jnp.float32)
    final_state, all_fields = lax.scan(advance, zero_state, (inverses, couplings, sources, counts.astype(jnp.int32)))
    return all_fields
```

```python
import jax
import jax.numpy as jnp
from jax import lax
from jax.sharding import PartitionSpec as P

CHUNKS = 2


def exchange(shard, axis, bit):
    count = lax.axis_size(axis)
    return lax.ppermute(shard, axis, [(i, i ^ bit) for i in range(count)])


def real_product(left_side, right_side):
    return jnp.dot(
        left_side, right_side, precision=lax.Precision.HIGH, preferred_element_type=jnp.float32
    )


def complex_product(left_side, right_side):
    gauss_sum = real_product(left_side[0] + left_side[1], right_side[0])
    gauss_diff = real_product(left_side[0], right_side[1] - right_side[0])
    gauss_cross = real_product(left_side[1], right_side[0] + right_side[1])
    return jnp.stack([gauss_sum - gauss_cross, gauss_sum + gauss_diff])


def in_order(pieces, place):
    bit = 1
    while len(pieces) > 1:
        upper = (place & bit) != 0
        joined = []
        for low, high in zip(pieces[0::2], pieces[1::2]):
            joined.append(
                jnp.concatenate(
                    [jnp.where(upper, high, low), jnp.where(upper, low, high)], axis=2
                )
            )
        pieces = joined
        bit *= 2
    return pieces[0]


def gathered(own):
    pieces = [own]
    bit = lax.axis_size("col") // 2
    parts = {0: own}
    while bit >= 1:
        parts.update({t ^ bit: exchange(v, "col", bit) for t, v in list(parts.items())})
        bit //= 2
    return [parts[t] for t in range(lax.axis_size("col"))]


def local(inverses, couplings, sources, counts):
    own_inverse, own_coupling, own_source = inverses[0], couplings[0], sources[0]
    orbitals = own_inverse.shape[1]
    width = own_source.shape[2]
    half = width // 2
    active = (lax.iota(jnp.int32, orbitals) < counts[0]).astype(jnp.float32)[:, None]
    chain_place = lax.axis_index("chain")
    chain_length = lax.axis_size("chain")
    col_place = lax.axis_index("col")
    odd = (chain_place & 1) == 1

    inverse = in_order(gathered(own_inverse), col_place)
    own_map = complex_product(inverse, own_coupling) * active
    offset = complex_product(inverse, own_source) * active

    other_map = exchange(own_map, "chain", 1)
    kept = jnp.where(odd, offset[:, :, half:], offset[:, :, :half])
    sent = jnp.where(odd, offset[:, :, :half], offset[:, :, half:])
    got = exchange(sent, "chain", 1)
    same = in_order(gathered(own_map), col_place)
    other = in_order(gathered(other_map), col_place)
    first_map = jnp.where(odd, other, same)
    second_map = jnp.where(odd, same, other)
    first_offset = jnp.where(odd, got, kept)
    second_offset = jnp.where(odd, kept, got)

    step = half // CHUNKS
    outs = []
    hops = chain_length // 2 - 1
    states = []
    for c in range(CHUNKS):
        a = first_offset[:, :, c * step:(c + 1) * step]
        b = second_offset[:, :, c * step:(c + 1) * step]
        states.append([a, b, jnp.zeros_like(a), a, complex_product(second_map, a) + b])
    for hop in range(hops):
        pairs = [(2 * hop + i, 2 * hop + 2 + i) for i in range(2)]
        for state in states:
            a, b, come, _, last = state
            come = come + lax.ppermute(last, "chain", pairs)
            first = complex_product(first_map, come) + a
            second = complex_product(second_map, first) + b
            state[2:] = [come, first, second]
    for state in states:
        first, second = state[3:]
        back = exchange(jnp.where(odd, first, second), "chain", 1)
        outs.append((jnp.where(odd, back, first), jnp.where(odd, second, back)))
    return jnp.concatenate([o[0] for o in outs] + [o[1] for o in outs], axis=2)[None]


def solution(mesh):
    placed = (
        P("chain", None, None, "col"),
        P("chain", None, None, "col"),
        P("chain", None, None, "col"),
        P("chain"),
    )
    return jax.shard_map(
        local, mesh=mesh, in_specs=placed, out_specs=P("chain", None, None, "col"), check_vma=False
    )
```

```python
import functools

import jax
import jax.numpy as jnp
from jax import lax
from jax.experimental import pallas as pl
from jax.experimental.pallas import tpu as pltpu
from jax.sharding import PartitionSpec as P

CHUNKS = 2
ROW_CHUNKS = 2
BF16, F32 = jnp.bfloat16, jnp.float32
WHOLE = pl.BlockSpec(memory_space=pltpu.VMEM)
SCALARS = pl.BlockSpec(memory_space=pltpu.SMEM)


def exchange(shard, axis, bit):
    count = lax.axis_size(axis)
    return lax.ppermute(shard, axis, [(i, i ^ bit) for i in range(count)])


def gathered(own):
    bit = lax.axis_size("col") // 2
    parts = {0: own}
    while bit >= 1:
        parts.update({t ^ bit: exchange(v, "col", bit) for t, v in list(parts.items())})
        bit //= 2
    return [parts[t] for t in range(lax.axis_size("col"))]


def kernel_call(kernel, scalars, arrays, outs, flops):
    return pl.pallas_call(
        kernel,
        out_shape=[jax.ShapeDtypeStruct(s, d) for s, d in outs],
        in_specs=[SCALARS] + [WHOLE] * len(arrays),
        out_specs=[WHOLE] * len(outs),
        compiler_params=pltpu.CompilerParams(vmem_limit_bytes=24 * 2**20),
        cost_estimate=pl.CostEstimate(flops=flops, bytes_accessed=4096, transcendentals=0),
    )(scalars, *arrays)


def split(value):
    high = value.astype(BF16)
    return high, (value - high.astype(F32)).astype(BF16)


def three_pass(left, right, dims):
    dot = functools.partial(lax.dot_general, dimension_numbers=(dims, ((), ())), preferred_element_type=F32)
    return dot(left[0], right[0]) + (dot(left[1], right[0]) + dot(left[0], right[1]))


def both_forms(real, imag):
    return jnp.concatenate(
        [jnp.concatenate([real, -imag], axis=1), jnp.concatenate([imag, real], axis=1)], axis=0
    )


def masked(value, start, count):
    lane = start + lax.broadcasted_iota(jnp.int32, value.shape, 1)
    return jnp.where(lane < count, value, 0.0)


def piece_order(ref, block, place, pieces):
    return jnp.concatenate(
        [ref[:, pl.ds(pl.multiple_of((place ^ t) * block, block), block)] for t in range(pieces)], axis=1
    )


def inverse_product(start, pieces, scal, left, *refs):
    parts = refs[:pieces]
    block = parts[0].shape[2]
    place, count = scal[0], scal[1]
    width = left.shape[1]
    ordered = [piece_order(left.at[i], block, place, pieces) for i in range(2)]
    right = jnp.concatenate([p[i] for i in range(2) for p in parts], axis=1)
    value = three_pass(split(both_forms(*ordered)), split(right), ((1,), (1,)))
    value = masked(value, start, count)
    return width, value


def map_kernel(start, pieces, scal, left, *refs):
    width, value = inverse_product(start, pieces, scal, left, *refs)
    out = refs[pieces]
    out[0] = value[:width]
    out[1] = value[width:]


def offset_kernel(row_chunks, pieces, chunks, scal, left, *refs):
    parts, outs = refs[:row_chunks * pieces], refs[row_chunks * pieces:]
    rows = parts[0].shape[1]
    half = left.shape[1] // 2
    step = half // chunks
    odd = scal[2]
    for r in range(row_chunks):
        for side in range(2):
            first = pl.multiple_of(jnp.where(odd == side, 0, half), half)
            rows_of = left.at[:, pl.ds(first, half)]
            width, value = inverse_product(
                r * rows, pieces, scal, rows_of, *parts[r * pieces:(r + 1) * pieces]
            )
            for c in range(chunks):
                for i in range(2):
                    outs[side * chunks + c][i, :, r * rows:(r + 1) * rows] = value[
                        i * width + c * step:i * width + (c + 1) * step
                    ]


def pack_kernel(row_chunks, pieces, scal, *refs):
    parts, (high, low) = refs[:-2], refs[-2:]
    block, rows = parts[0].shape[1:]
    place, odd = scal[0], scal[2]
    size = block * pieces
    for which in range(2):
        slot = jnp.where(which == 0, odd, 1 - odd)
        for r in range(row_chunks):
            for t in range(pieces):
                part = parts[(which * row_chunks + r) * pieces + t]
                for i in range(2):
                    at = pl.ds(pl.multiple_of((place ^ t) * block + i * size, block), block)
                    high_part, low_part = split(part[i])
                    high[slot, at, r * rows:(r + 1) * rows] = high_part
                    low[slot, at, r * rows:(r + 1) * rows] = low_part


def apply_map(slot, high, low, state):
    count = state.shape[0] // 2
    value = three_pass(
        split(both_forms(state[:count], state[count:])), (high[slot], low[slot]), ((1,), (0,))
    )
    return value


def stacked(ref):
    return jnp.concatenate([ref[0], ref[1]], axis=0)


def stage_kernel(mode, scal, high, low, kept, got, *refs):
    odd = scal[2] == 1
    mine, theirs = stacked(kept), stacked(got)
    first = jnp.where(odd, theirs, mine)
    second = jnp.where(odd, mine, theirs)
    if mode == "first":
        come, outs = None, refs
    elif mode == "middle":
        come, outs = stacked(refs[0]), refs[1:]
    else:
        come, outs = stacked(refs[0]) + stacked(refs[1]), refs[2:]
    if come is not None:
        first = first + apply_map(0, high, low, come)
    second = second + apply_map(1, high, low, first)
    count = kept.shape[1]
    if mode == "last":
        values = [jnp.where(odd, second, first), jnp.where(odd, first, second)]
    else:
        values = [second]
    for out, value in zip(outs, values):
        out[0] = value[:count]
        out[1] = value[count:]


def final_kernel(chunks, scal, *refs):
    keep, back, out = refs[:chunks], refs[chunks:-1], refs[-1]
    half = out.shape[2] // 2
    odd = scal[2]
    for side, pieces in ((0, keep), (1, back)):
        first = pl.multiple_of(jnp.where(odd == side, 0, half), half)
        for i in range(2):
            whole = jnp.concatenate([p[i] for p in pieces], axis=0)
            out[i, :, pl.ds(first, half)] = whole.T


def body(inverses, couplings, sources, counts):
    own_inverse, own_coupling, own_source = inverses[0], couplings[0], sources[0]
    orbitals, block = own_inverse.shape[1:]
    width = own_source.shape[2]
    half = width // 2
    step = half // CHUNKS
    pieces = lax.axis_size("col")
    chain_place = lax.axis_index("chain")
    chain_length = lax.axis_size("chain")
    col_place = lax.axis_index("col")
    scal = jnp.stack([col_place.astype(jnp.int32), counts[0], (chain_place & 1).astype(jnp.int32)])
    rows = orbitals // ROW_CHUNKS
    coupling_t = jnp.swapaxes(own_coupling, 1, 2)
    source_t = jnp.swapaxes(own_source, 1, 2)

    inverse, same, other = [], [], []
    for r in range(ROW_CHUNKS):
        parts = gathered(own_inverse[:, r * rows:(r + 1) * rows])
        inverse += parts
        (own_map,) = kernel_call(
            functools.partial(map_kernel, r * rows, pieces),
            scal,
            [coupling_t, *parts],
            [((2, block, rows), F32)],
            8 * rows * block * orbitals,
        )
        other_map = exchange(own_map, "chain", 1)
        same += gathered(own_map)
        other += gathered(other_map)
    shape = (2, step, orbitals)
    offsets = kernel_call(
        functools.partial(offset_kernel, ROW_CHUNKS, pieces, CHUNKS),
        scal,
        [source_t, *inverse],
        [(shape, F32)] * (2 * CHUNKS),
        8 * orbitals * orbitals * width,
    )
    kept, sent = offsets[:CHUNKS], offsets[CHUNKS:]
    packed = (2, 2 * orbitals, orbitals)
    high, low = kernel_call(
        functools.partial(pack_kernel, ROW_CHUNKS, pieces),
        scal,
        [*same, *other],
        [(packed, BF16)] * 2,
        8 * orbitals * orbitals,
    )
    hops = chain_length // 2 - 1
    flops = 16 * orbitals * orbitals * step
    got, last, come = [], [], [[] for _ in range(CHUNKS)]
    for c in range(CHUNKS):
        got.append(exchange(sent[c], "chain", 1))
        last += kernel_call(
            functools.partial(stage_kernel, "first"),
            scal,
            [high, low, kept[c], got[c]],
            [(shape, F32)],
            flops // 2,
        )
    keep, back = [], []
    for hop in range(hops):
        pairs = [(2 * hop + i, 2 * hop + 2 + i) for i in range(2)]
        for c in range(CHUNKS):
            arrived = lax.ppermute(last[c], "chain", pairs)
            final = hop == hops - 1
            earlier = come[c]
            come[c] = arrived if hop == 0 else earlier + arrived
            if final:
                inputs = [earlier if hop else jnp.zeros_like(arrived), arrived]
            else:
                inputs = [arrived]
            results = kernel_call(
                functools.partial(stage_kernel, "last" if final else "middle"),
                scal,
                [high, low, kept[c], got[c], *inputs],
                [(shape, F32)] * (2 if final else 1),
                flops,
            )
            if final:
                keep.append(results[0])
                back.append(exchange(results[1], "chain", 1))
            else:
                last[c] = results[0]
    (out,) = kernel_call(
        functools.partial(final_kernel, CHUNKS),
        scal,
        [*keep, *back],
        [((2, orbitals, width), F32)],
        orbitals * width,
    )
    return out[None]


def solution(mesh):
    placed = (
        P("chain", None, None, "col"),
        P("chain", None, None, "col"),
        P("chain", None, None, "col"),
        P("chain"),
    )
    return jax.shard_map(
        body, mesh=mesh, in_specs=placed, out_specs=P("chain", None, None, "col"), check_vma=False
    )
```

```python
import functools

import jax
import jax.numpy as jnp
from jax import lax
from jax.experimental import pallas as pl
from jax.experimental.pallas import tpu as pltpu
from jax.sharding import PartitionSpec as P

PARTS = (2, 3, 3)
CHUNKS = len(PARTS)
ROW_CHUNKS = 2
BF16, F32 = jnp.bfloat16, jnp.float32
WHOLE = pl.BlockSpec(memory_space=pltpu.VMEM)


def column_spans(width):
    cuts = [-(-width * sum(PARTS[:c]) // (8 * sum(PARTS))) * 8 for c in range(CHUNKS + 1)]
    return list(zip(cuts, cuts[1:]))


def exchange(shard, axis, bit):
    count = lax.axis_size(axis)
    return lax.ppermute(shard, axis, [(i, i ^ bit) for i in range(count)])


def gathered(own):
    bit = lax.axis_size("col") // 2
    parts = {0: own}
    while bit >= 1:
        parts.update({t ^ bit: exchange(v, "col", bit) for t, v in list(parts.items())})
        bit //= 2
    return [parts[t] for t in range(lax.axis_size("col"))]


def kernel_call(kernel, arrays, outs, flops):
    return pl.pallas_call(
        kernel,
        out_shape=[jax.ShapeDtypeStruct(s, d) for s, d in outs],
        in_specs=[WHOLE] * len(arrays),
        out_specs=[WHOLE] * len(outs),
        compiler_params=pltpu.CompilerParams(vmem_limit_bytes=24 * 2**20),
        cost_estimate=pl.CostEstimate(flops=flops, bytes_accessed=4096, transcendentals=0),
    )(*arrays)


def col_place():
    return lax.axis_index("col").astype(jnp.int32)


def chain_half():
    return lax.axis_index("chain").astype(jnp.int32) & 1


def split(value):
    high = value.astype(BF16)
    return high, (value - high.astype(F32)).astype(BF16)


def three_pass(left, right, dims):
    dot = functools.partial(lax.dot_general, dimension_numbers=(dims, ((), ())), preferred_element_type=F32)
    return dot(left[0], right[0]) + (dot(left[1], right[0]) + dot(left[0], right[1]))


def both_forms(real, imag):
    return jnp.concatenate(
        [jnp.concatenate([real, -imag], axis=1), jnp.concatenate([imag, real], axis=1)], axis=0
    )


def masked(value, active):
    return jnp.where(active > 0.0, value, 0.0)


def couple_kernel(pieces, natural, high, low):
    size = natural.shape[1]
    block = size // pieces
    place = col_place()
    ordered = []
    for i in range(2):
        rows = [
            natural[i, pl.ds(pl.multiple_of((place ^ t) * block, block), block)]
            for t in range(pieces)
        ]
        ordered.append(jnp.concatenate(rows, axis=0).T)
    high[...], low[...] = split(both_forms(*ordered))


def source_kernel(pieces, natural, high, low):
    size, width = natural.shape[1:]
    block, half = size // pieces, width // 2
    place, odd = col_place(), chain_half()
    for side in range(2):
        first = pl.multiple_of(jnp.where(odd == side, 0, half), half)
        ordered = []
        for i in range(2):
            rows = [
                natural[i, pl.ds(pl.multiple_of((place ^ t) * block, block), block), pl.ds(first, half)]
                for t in range(pieces)
            ]
            ordered.append(jnp.concatenate(rows, axis=0).T)
        high[side], low[side] = split(both_forms(*ordered))


def inverse_product(left, parts):
    right = jnp.concatenate([p[i] for i in range(2) for p in parts], axis=1)
    return three_pass(left, split(right), ((1,), (1,)))


def columns_of(refs, first, count):
    half = refs[0].shape[1] // 2
    return [
        jnp.concatenate([ref[:, i * half + first:i * half + first + count] for i in range(2)], axis=1)
        for ref in refs
    ]


def near_kernel(high, low, *refs):
    parts, out = refs[:-1], refs[-1]
    count = sum(p.shape[2] for p in parts)
    out[...] = inverse_product(columns_of((high, low), 0, count), parts)


def map_kernel(start, active, high, low, near, *refs):
    parts, out = refs[:-1], refs[-1]
    count = sum(p.shape[2] for p in parts)
    left = columns_of((high, low), high.shape[1] // 2 - count, count)
    width, rows = out.shape[1:]
    value = masked(near[...] + inverse_product(left, parts), active[:1, start:start + rows])
    out[0] = value[:width]
    out[1] = value[width:]


def offset_kernel(row_chunks, pieces, spans, active, high, low, *refs):
    parts, outs = refs[:row_chunks * pieces], refs[row_chunks * pieces:]
    rows = parts[0].shape[1]
    half = high.shape[1] // 2
    left = [jnp.concatenate([ref[0], ref[1]], axis=0) for ref in (high, low)]
    for r in range(row_chunks):
        value = inverse_product(left, parts[r * pieces:(r + 1) * pieces])
        value = masked(value, active[:1, r * rows:(r + 1) * rows])
        for side in range(2):
            for c, (low_end, high_end) in enumerate(spans):
                for i in range(2):
                    at = (2 * side + i) * half
                    out = outs[side * len(spans) + c]
                    out[i, :, r * rows:(r + 1) * rows] = value[at + low_end:at + high_end]


def pack_kernel(pieces, *refs):
    parts, (high, low) = refs[:-2], refs[-2:]
    block = parts[0].shape[1]
    place, odd = col_place(), chain_half()
    size = block * pieces
    for which in range(2):
        slot = odd if which == 0 else 1 - odd
        for t in range(pieces):
            part = parts[which * pieces + t]
            for i in range(2):
                at = pl.ds(pl.multiple_of((place ^ t) * block + i * size, block), block)
                high[slot, at, :], low[slot, at, :] = split(part[i])


def forms_of(value):
    count = value.shape[0] // 2
    return split(both_forms(value[:count], value[count:]))


def apply_map(left, pair):
    (high, low), (right_high, right_low) = left, pair
    count = high.shape[0]
    dot = functools.partial(jnp.dot, preferred_element_type=F32)
    both = dot(jnp.concatenate([high, low], axis=0), right_high)
    return both[:count] + (both[count:] + dot(high, right_low))


def stacked(ref):
    return jnp.concatenate([ref[0], ref[1]], axis=0)


def put(ref, value, at=slice(None)):
    count = value.shape[0] // 2
    ref[0, :, at] = value[:count]
    ref[1, :, at] = value[count:]


def row_pairs(packs, slot):
    count = len(packs) // 2
    return [(packs[r][slot], packs[count + r][slot]) for r in range(count)]


def apply_maps(left, packs, slot):
    return jnp.concatenate([apply_map(left, pair) for pair in row_pairs(packs, slot)], axis=1)


def stage_kernel(hop, final, kept, got, *refs):
    before, refs = (refs[:3], refs[3:]) if hop else ((), refs)
    packs, outs = (refs[:-2], refs[-2:]) if final else (refs[:-3], refs[-3:])
    turn = lax.axis_index("chain").astype(jnp.int32) >> 1 == hop

    @pl.when(turn)
    def _():
        odd = chain_half() == 1
        mine, theirs = stacked(kept), stacked(got)
        first = jnp.where(odd, theirs, mine)
        if hop:
            first = first + apply_maps(forms_of(stacked(before[0])), packs, 0)
        second = jnp.where(odd, mine, theirs) + apply_maps(forms_of(first), packs, 1)
        if not final:
            put(outs[0], second)
        put(outs[-2], jnp.where(odd, second, first))
        put(outs[-1], jnp.where(odd, first, second))

    if hop:

        @pl.when(jnp.logical_not(turn))
        def _():
            outs[-2][...] = before[1][...]
            outs[-1][...] = before[2][...]


def half_kernel(side, chunks, *refs):
    parts, (out, block, sems) = refs[:chunks], refs[-3:]
    half = block.shape[2]
    first = pl.multiple_of(jnp.where(chain_half() == side, 0, half), half)
    copies = []
    for i in range(2):
        block[i] = jnp.concatenate([p[i] for p in parts], axis=0).T
        copies.append(pltpu.make_async_copy(block.at[i], out.at[i, :, pl.ds(first, half)], sems.at[i]))
        copies[i].start()
    for copy in copies:
        copy.wait()


def body(inverses, couplings, sources, counts):
    own_inverse, own_coupling, own_source = inverses[0], couplings[0], sources[0]
    orbitals, block = own_inverse.shape[1:]
    width = own_source.shape[2]
    half = width // 2
    spans = column_spans(half)
    pieces = lax.axis_size("col")
    far = pieces // 2
    chain_length = lax.axis_size("chain")
    active = (lax.broadcasted_iota(jnp.int32, (8, orbitals), 1) < counts[0]).astype(F32)
    rows = orbitals // ROW_CHUNKS
    flops = 8 * orbitals * orbitals

    couple = kernel_call(
        functools.partial(couple_kernel, pieces),
        [own_coupling],
        [((2 * block, 2 * orbitals), BF16)] * 2,
        flops,
    )
    source = kernel_call(
        functools.partial(source_kernel, pieces),
        [own_source],
        [((2, width, 2 * orbitals), BF16)] * 2,
        flops,
    )
    inverse, packs = [], []
    for r in range(ROW_CHUNKS):
        source_rows = lax.optimization_barrier(own_inverse) if r else own_inverse
        parts = gathered(source_rows[:, r * rows:(r + 1) * rows])
        inverse += parts
        (near,) = kernel_call(
            near_kernel, [*couple, *parts[:far]], [((2 * block, rows), F32)], flops * block
        )
        (own_map,) = kernel_call(
            functools.partial(map_kernel, r * rows),
            [active, *couple, near, *parts[far:]],
            [((2, block, rows), F32)],
            flops * block // ROW_CHUNKS,
        )
        same = gathered(own_map)
        other_map = exchange(own_map, "chain", 1)
        if r % 2 == 0:
            other = [other_map] + [None] * (pieces - 1)
            for t in range(1, far):
                other[t] = exchange(other_map, "col", t)
            for t in range(far, pieces):
                if t == far:
                    other[t] = exchange(same[t], "chain", 1)
                else:
                    other[t] = exchange(other[far], "col", t ^ far)
        else:
            other = gathered(other_map)
        packs.append(
            kernel_call(
                functools.partial(pack_kernel, pieces),
                    [*same, *other],
                [((2, 2 * orbitals, rows), BF16)] * 2,
                flops,
            )
        )
    packs = [p[0] for p in packs] + [p[1] for p in packs]
    shapes = [(2, end - start, orbitals) for start, end in spans]
    offsets = kernel_call(
        functools.partial(offset_kernel, ROW_CHUNKS, pieces, spans),
        [active, *source, *inverse],
        [(shape, F32) for shape in shapes] * 2,
        flops * width,
    )
    kept, sent = offsets[:CHUNKS], offsets[CHUNKS:]
    hops = chain_length // 2 - 1
    got = [exchange(sent[c], "chain", 1) for c in range(CHUNKS)]
    held = [[] for _ in range(CHUNKS)]
    keep, back = [], []
    for hop in range(hops + 1):
        final = hop == hops
        pairs = [(2 * hop + i, 2 * hop + 2 + i) for i in range(2)]
        for c in range(CHUNKS):
            *passed, mine, theirs = kernel_call(
                functools.partial(stage_kernel, hop, final),
                    [kept[c], got[c], *held[c], *packs],
                [(shapes[c], F32)] * (2 if final else 3),
                flops * half,
            )
            if final:
                keep.append(mine)
                back.append(exchange(theirs, "chain", 1))
            else:
                held[c] = [lax.ppermute(passed[0], "chain", pairs), mine, theirs]
    out = None
    for side, parts in enumerate((keep, back)):
        out = pl.pallas_call(
            functools.partial(half_kernel, side, CHUNKS),
            out_shape=jax.ShapeDtypeStruct((2, orbitals, width), F32),
            in_specs=[WHOLE] * CHUNKS + [pl.BlockSpec(memory_space=pl.ANY)] * side,
            out_specs=pl.BlockSpec(memory_space=pl.ANY),
            scratch_shapes=[pltpu.VMEM((2, orbitals, half), F32), pltpu.SemaphoreType.DMA((2,))],
            input_output_aliases={CHUNKS: 0} if side else {},
            compiler_params=pltpu.CompilerParams(vmem_limit_bytes=24 * 2**20),
            cost_estimate=pl.CostEstimate(flops=flops, bytes_accessed=4096, transcendentals=0),
        )(*parts, *([out] if side else []))
    return out[None]


def solution(mesh):
    placed = (
        P("chain", None, None, "col"),
        P("chain", None, None, "col"),
        P("chain", None, None, "col"),
        P("chain"),
    )
    return jax.shard_map(
        body, mesh=mesh, in_specs=placed, out_specs=P("chain", None, None, "col"), check_vma=False
    )
```

```python
import functools

import jax
import jax.numpy as jnp
from jax import lax
from jax.experimental import pallas as pl
from jax.experimental.pallas import tpu as pltpu
from jax.sharding import PartitionSpec as P

PARTS = (1, 1, 1, 1)
CHUNKS = len(PARTS)
ROW_CHUNKS = 2
BF16, F32 = jnp.bfloat16, jnp.float32
WHOLE = pl.BlockSpec(memory_space=pltpu.VMEM)


def column_spans(width):
    cuts = [-(-width * sum(PARTS[:c]) // (8 * sum(PARTS))) * 8 for c in range(CHUNKS + 1)]
    return list(zip(cuts, cuts[1:]))


def exchange(shard, axis, bit):
    count = lax.axis_size(axis)
    return lax.ppermute(shard, axis, [(i, i ^ bit) for i in range(count)])


def gathered(own):
    bit = lax.axis_size("col") // 2
    parts = {0: own}
    while bit >= 1:
        parts.update({t ^ bit: exchange(v, "col", bit) for t, v in list(parts.items())})
        bit //= 2
    return [parts[t] for t in range(lax.axis_size("col"))]


def kernel_call(kernel, arrays, outs, flops):
    return pl.pallas_call(
        kernel,
        out_shape=[jax.ShapeDtypeStruct(s, d) for s, d in outs],
        in_specs=[WHOLE] * len(arrays),
        out_specs=[WHOLE] * len(outs),
        compiler_params=pltpu.CompilerParams(vmem_limit_bytes=24 * 2**20),
        cost_estimate=pl.CostEstimate(flops=flops, bytes_accessed=4096, transcendentals=0),
    )(*arrays)


def col_place():
    return lax.axis_index("col").astype(jnp.int32)


def chain_half():
    return lax.axis_index("chain").astype(jnp.int32) & 1


def split(value):
    high = value.astype(BF16)
    return high, (value - high.astype(F32)).astype(BF16)


def three_pass(left, right, dims):
    dot = functools.partial(lax.dot_general, dimension_numbers=(dims, ((), ())), preferred_element_type=F32)
    return dot(left[0], right[0]) + (dot(left[1], right[0]) + dot(left[0], right[1]))


def both_forms(real, imag):
    return jnp.concatenate(
        [jnp.concatenate([real, -imag], axis=1), jnp.concatenate([imag, real], axis=1)], axis=0
    )


def masked(value, active):
    return jnp.where(active > 0.0, value, 0.0)


def couple_kernel(pieces, natural, high, low):
    size = natural.shape[1]
    block = size // pieces
    place = col_place()
    ordered = []
    for i in range(2):
        rows = [
            natural[i, pl.ds(pl.multiple_of((place ^ t) * block, block), block)]
            for t in range(pieces)
        ]
        ordered.append(jnp.concatenate(rows, axis=0).T)
    high[...], low[...] = split(both_forms(*ordered))


def source_kernel(pieces, natural, high, low):
    size, width = natural.shape[1:]
    block, half = size // pieces, width // 2
    place, odd = col_place(), chain_half()
    for side in range(2):
        first = pl.multiple_of(jnp.where(odd == side, 0, half), half)
        ordered = []
        for i in range(2):
            rows = [
                natural[i, pl.ds(pl.multiple_of((place ^ t) * block, block), block), pl.ds(first, half)]
                for t in range(pieces)
            ]
            ordered.append(jnp.concatenate(rows, axis=0).T)
        high[side], low[side] = split(both_forms(*ordered))


def inverse_product(left, parts):
    right = jnp.concatenate([p[i] for i in range(2) for p in parts], axis=1)
    return three_pass(left, split(right), ((1,), (1,)))


def columns_of(refs, first, count):
    half = refs[0].shape[1] // 2
    return [
        jnp.concatenate([ref[:, i * half + first:i * half + first + count] for i in range(2)], axis=1)
        for ref in refs
    ]


def near_kernel(high, low, *refs):
    parts, out = refs[:-1], refs[-1]
    count = sum(p.shape[2] for p in parts)
    out[...] = inverse_product(columns_of((high, low), 0, count), parts)


def map_kernel(start, active, high, low, near, *refs):
    parts, out = refs[:-1], refs[-1]
    count = sum(p.shape[2] for p in parts)
    left = columns_of((high, low), high.shape[1] // 2 - count, count)
    width, rows = out.shape[1:]
    value = masked(near[...] + inverse_product(left, parts), active[:1, start:start + rows])
    out[0] = value[:width]
    out[1] = value[width:]


def offset_kernel(row_chunks, pieces, spans, active, high, low, *refs):
    parts, outs = refs[:row_chunks * pieces], refs[row_chunks * pieces:]
    rows = parts[0].shape[1]
    half = high.shape[1] // 2
    left = [jnp.concatenate([ref[0], ref[1]], axis=0) for ref in (high, low)]
    for r in range(row_chunks):
        value = inverse_product(left, parts[r * pieces:(r + 1) * pieces])
        value = masked(value, active[:1, r * rows:(r + 1) * rows])
        for side in range(2):
            for c, (low_end, high_end) in enumerate(spans):
                for i in range(2):
                    at = (2 * side + i) * half
                    out = outs[side * len(spans) + c]
                    out[i, :, r * rows:(r + 1) * rows] = value[at + low_end:at + high_end]


def pack_kernel(pieces, *refs):
    parts, (high, low) = refs[:-2], refs[-2:]
    block = parts[0].shape[1]
    place, odd = col_place(), chain_half()
    size = block * pieces
    for which in range(2):
        slot = odd if which == 0 else 1 - odd
        for t in range(pieces):
            part = parts[which * pieces + t]
            for i in range(2):
                at = pl.ds(pl.multiple_of((place ^ t) * block + i * size, block), block)
                high[slot, at, :], low[slot, at, :] = split(part[i])


def forms_of(value):
    count = value.shape[0] // 2
    return split(both_forms(value[:count], value[count:]))


def apply_map(left, pair):
    (high, low), (right_high, right_low) = left, pair
    count = high.shape[0]
    dot = functools.partial(jnp.dot, preferred_element_type=F32)
    both = dot(jnp.concatenate([high, low], axis=0), right_high)
    return both[:count] + (both[count:] + dot(high, right_low))


def stacked(ref):
    return jnp.concatenate([ref[0], ref[1]], axis=0)


def put(ref, value, at=slice(None)):
    count = value.shape[0] // 2
    ref[0, :, at] = value[:count]
    ref[1, :, at] = value[count:]


def row_pairs(packs, slot):
    count = len(packs) // 2
    return [(packs[r][slot], packs[count + r][slot]) for r in range(count)]


def apply_maps(left, packs, slot):
    return jnp.concatenate([apply_map(left, pair) for pair in row_pairs(packs, slot)], axis=1)


def stage_kernel(hop, final, early, kept, got, *refs):
    count = (2 if early else 3) if hop else 0
    before, refs = refs[:count], refs[count:]
    packs, outs = (refs[:-2], refs[-2:]) if final else (refs[:-3], refs[-3:])
    turn = lax.axis_index("chain").astype(jnp.int32) >> 1 == hop

    @pl.when(turn)
    def _():
        odd = chain_half() == 1
        mine, theirs = stacked(kept), stacked(got)
        first = jnp.where(odd, theirs, mine)
        if hop:
            first = first + apply_maps(forms_of(stacked(before[0])), packs, 0)
        second = jnp.where(odd, mine, theirs) + apply_maps(forms_of(first), packs, 1)
        if not final:
            put(outs[0], second)
        put(outs[-2], jnp.where(odd, second, first))
        put(outs[-1], jnp.where(odd, first, second))

    if hop:

        @pl.when(jnp.logical_not(turn))
        def _():
            outs[-2][...] = before[1][...]
            if not early:
                outs[-1][...] = before[2][...]


def half_kernel(side, chunks, hops, *refs):
    parts, (out, block, sems) = refs[:-3 - side], refs[-3:]
    half = block.shape[2]
    first = pl.multiple_of(jnp.where(chain_half() == side, 0, half), half)
    last = lax.axis_index("chain").astype(jnp.int32) >> 1 == hops
    copies = []
    for i in range(2):
        pieces = [p[i] for p in parts]
        if len(pieces) > chunks:
            pieces = [jnp.where(last, pieces[1], pieces[0])] + pieces[2:]
        block[i] = jnp.concatenate(pieces, axis=0).T
        copies.append(pltpu.make_async_copy(block.at[i], out.at[i, :, pl.ds(first, half)], sems.at[i]))
        copies[i].start()
    for copy in copies:
        copy.wait()


def body(inverses, couplings, sources, counts):
    own_inverse, own_coupling, own_source = inverses[0], couplings[0], sources[0]
    orbitals, block = own_inverse.shape[1:]
    width = own_source.shape[2]
    half = width // 2
    spans = column_spans(half)
    pieces = lax.axis_size("col")
    far = pieces // 2
    chain_length = lax.axis_size("chain")
    active = (lax.broadcasted_iota(jnp.int32, (8, orbitals), 1) < counts[0]).astype(F32)
    rows = orbitals // ROW_CHUNKS
    flops = 8 * orbitals * orbitals

    couple = kernel_call(
        functools.partial(couple_kernel, pieces),
        [own_coupling],
        [((2 * block, 2 * orbitals), BF16)] * 2,
        flops,
    )
    source = kernel_call(
        functools.partial(source_kernel, pieces),
        [own_source],
        [((2, width, 2 * orbitals), BF16)] * 2,
        flops,
    )
    inverse, packs = [], []
    for r in range(ROW_CHUNKS):
        source_rows = lax.optimization_barrier(own_inverse) if r else own_inverse
        parts = gathered(source_rows[:, r * rows:(r + 1) * rows])
        inverse += parts
        (near,) = kernel_call(
            near_kernel, [*couple, *parts[:far]], [((2 * block, rows), F32)], flops * block
        )
        (own_map,) = kernel_call(
            functools.partial(map_kernel, r * rows),
            [active, *couple, near, *parts[far:]],
            [((2, block, rows), F32)],
            flops * block // ROW_CHUNKS,
        )
        same = gathered(own_map)
        other_map = exchange(own_map, "chain", 1)
        if r % 2 == 0:
            other = [other_map] + [None] * (pieces - 1)
            for t in range(1, far):
                other[t] = exchange(other_map, "col", t)
            for t in range(far, pieces):
                if t == far:
                    other[t] = exchange(same[t], "chain", 1)
                else:
                    other[t] = exchange(other[far], "col", t ^ far)
        else:
            other = gathered(other_map)
        packs.append(
            kernel_call(
                functools.partial(pack_kernel, pieces),
                    [*same, *other],
                [((2, 2 * orbitals, rows), BF16)] * 2,
                flops,
            )
        )
    packs = [p[0] for p in packs] + [p[1] for p in packs]
    shapes = [(2, end - start, orbitals) for start, end in spans]
    offsets = kernel_call(
        functools.partial(offset_kernel, ROW_CHUNKS, pieces, spans),
        [active, *source, *inverse],
        [(shape, F32) for shape in shapes] * 2,
        flops * width,
    )
    kept, sent = offsets[:CHUNKS], offsets[CHUNKS:]
    hops = chain_length // 2 - 1
    got = [exchange(sent[c], "chain", 1) for c in range(CHUNKS)]
    held = [[] for _ in range(CHUNKS)]
    keep, back = [], []
    for hop in range(hops + 1):
        final = hop == hops
        pairs = [(2 * hop + i, 2 * hop + 2 + i) for i in range(2)]
        for c in range(CHUNKS):
            *passed, mine, theirs = kernel_call(
                functools.partial(stage_kernel, hop, final, final and c == 0),
                    [kept[c], got[c], *held[c], *packs],
                [(shapes[c], F32)] * (2 if final else 3),
                flops * half,
            )
            if not final:
                held[c] = [lax.ppermute(passed[0], "chain", pairs), mine, theirs]
                if c == 0 and hop == hops - 1:
                    early = exchange(held[c].pop(), "chain", 1)
                continue
            keep.append(mine)
            if c == 0 and hops:
                own = [(2 * hops + i, 2 * hops + 1 - i) for i in range(2)]
                back += [early, lax.ppermute(theirs, "chain", own)]
            else:
                back.append(exchange(theirs, "chain", 1))
    out = None
    for side, parts in enumerate((keep, back)):
        out = pl.pallas_call(
            functools.partial(half_kernel, side, CHUNKS, hops),
            out_shape=jax.ShapeDtypeStruct((2, orbitals, width), F32),
            in_specs=[WHOLE] * len(parts) + [pl.BlockSpec(memory_space=pl.ANY)] * side,
            out_specs=pl.BlockSpec(memory_space=pl.ANY),
            scratch_shapes=[pltpu.VMEM((2, orbitals, half), F32), pltpu.SemaphoreType.DMA((2,))],
            input_output_aliases={len(parts): 0} if side else {},
            compiler_params=pltpu.CompilerParams(vmem_limit_bytes=24 * 2**20),
            cost_estimate=pl.CostEstimate(flops=flops, bytes_accessed=4096, transcendentals=0),
        )(*parts, *([out] if side else []))
    return out[None]


def solution(mesh):
    placed = (
        P("chain", None, None, "col"),
        P("chain", None, None, "col"),
        P("chain", None, None, "col"),
        P("chain"),
    )
    return jax.shard_map(
        body, mesh=mesh, in_specs=placed, out_specs=P("chain", None, None, "col"), check_vma=False
    )
```

```python
import functools

import jax
import jax.numpy as jnp
from jax import lax
from jax.experimental import pallas as pl
from jax.experimental.pallas import tpu as pltpu
from jax.sharding import PartitionSpec as P

PARTS = (1, 1, 1, 1)
CHUNKS = len(PARTS)
ROW_CHUNKS = 2
BF16, F32 = jnp.bfloat16, jnp.float32
WHOLE = pl.BlockSpec(memory_space=pltpu.VMEM)


def column_spans(width):
    cuts = [-(-width * sum(PARTS[:c]) // (8 * sum(PARTS))) * 8 for c in range(CHUNKS + 1)]
    return list(zip(cuts, cuts[1:]))


def exchange(shard, axis, bit):
    count = lax.axis_size(axis)
    return lax.ppermute(shard, axis, [(i, i ^ bit) for i in range(count)])


def between(shard, moves):
    chain, col = lax.axis_size("chain"), lax.axis_size("col")
    pairs = []
    for i in range(chain):
        for j in range(col):
            to = moves[i] * col + j if i in moves else i * col + (j ^ 1)
            pairs.append((i * col + j, to))
    return lax.ppermute(shard, ("chain", "col"), pairs)


def gathered(own):
    bit = lax.axis_size("col") // 2
    parts = {0: own}
    while bit >= 1:
        parts.update({t ^ bit: exchange(v, "col", bit) for t, v in list(parts.items())})
        bit //= 2
    return [parts[t] for t in range(lax.axis_size("col"))]


def kernel_call(kernel, arrays, outs, flops):
    return pl.pallas_call(
        kernel,
        out_shape=[jax.ShapeDtypeStruct(s, d) for s, d in outs],
        in_specs=[WHOLE] * len(arrays),
        out_specs=[WHOLE] * len(outs),
        compiler_params=pltpu.CompilerParams(vmem_limit_bytes=24 * 2**20),
        cost_estimate=pl.CostEstimate(flops=flops, bytes_accessed=4096, transcendentals=0),
    )(*arrays)


def col_place():
    return lax.axis_index("col").astype(jnp.int32)


def chain_half():
    return lax.axis_index("chain").astype(jnp.int32) & 1


def split(value):
    high = value.astype(BF16)
    return high, (value - high.astype(F32)).astype(BF16)


def three_pass(left, right, dims):
    dot = functools.partial(lax.dot_general, dimension_numbers=(dims, ((), ())), preferred_element_type=F32)
    return dot(left[0], right[0]) + (dot(left[1], right[0]) + dot(left[0], right[1]))


def both_forms(real, imag):
    return jnp.concatenate(
        [jnp.concatenate([real, -imag], axis=1), jnp.concatenate([imag, real], axis=1)], axis=0
    )


def masked(value, active):
    return jnp.where(active > 0.0, value, 0.0)


def couple_kernel(pieces, natural, high, low):
    size = natural.shape[1]
    block = size // pieces
    place = col_place()
    ordered = []
    for i in range(2):
        rows = [
            natural[i, pl.ds(pl.multiple_of((place ^ t) * block, block), block)]
            for t in range(pieces)
        ]
        ordered.append(jnp.concatenate(rows, axis=0).T)
    high[...], low[...] = split(both_forms(*ordered))


def source_kernel(pieces, natural, high, low):
    size, width = natural.shape[1:]
    block, half = size // pieces, width // 2
    place, odd = col_place(), chain_half()
    for side in range(2):
        first = pl.multiple_of(jnp.where(odd == side, 0, half), half)
        ordered = []
        for i in range(2):
            rows = [
                natural[i, pl.ds(pl.multiple_of((place ^ t) * block, block), block), pl.ds(first, half)]
                for t in range(pieces)
            ]
            ordered.append(jnp.concatenate(rows, axis=0).T)
        high[side], low[side] = split(both_forms(*ordered))


def inverse_product(left, parts):
    right = jnp.concatenate([p[i] for i in range(2) for p in parts], axis=1)
    return three_pass(left, split(right), ((1,), (1,)))


def columns_of(refs, first, count):
    half = refs[0].shape[1] // 2
    return [
        jnp.concatenate([ref[:, i * half + first:i * half + first + count] for i in range(2)], axis=1)
        for ref in refs
    ]


def near_kernel(high, low, *refs):
    parts, out = refs[:-1], refs[-1]
    count = sum(p.shape[2] for p in parts)
    out[...] = inverse_product(columns_of((high, low), 0, count), parts)


def map_kernel(start, active, high, low, near, *refs):
    parts, out = refs[:-1], refs[-1]
    count = sum(p.shape[2] for p in parts)
    left = columns_of((high, low), high.shape[1] // 2 - count, count)
    width, rows = out.shape[1:]
    value = masked(near[...] + inverse_product(left, parts), active[:1, start:start + rows])
    out[0] = value[:width]
    out[1] = value[width:]


def offset_kernel(row_chunks, pieces, spans, active, high, low, *refs):
    parts, outs = refs[:row_chunks * pieces], refs[row_chunks * pieces:]
    rows = parts[0].shape[1]
    half = high.shape[1] // 2
    left = [jnp.concatenate([ref[0], ref[1]], axis=0) for ref in (high, low)]
    for r in range(row_chunks):
        value = inverse_product(left, parts[r * pieces:(r + 1) * pieces])
        value = masked(value, active[:1, r * rows:(r + 1) * rows])
        for side in range(2):
            for c, (low_end, high_end) in enumerate(spans):
                for i in range(2):
                    at = (2 * side + i) * half
                    out = outs[side * len(spans) + c]
                    out[i, :, r * rows:(r + 1) * rows] = value[at + low_end:at + high_end]


def pack_kernel(pieces, *refs):
    parts, (high, low) = refs[:-2], refs[-2:]
    block = parts[0].shape[1]
    place, odd = col_place(), chain_half()
    size = block * pieces
    for which in range(2):
        slot = odd if which == 0 else 1 - odd
        for t in range(pieces):
            part = parts[which * pieces + t]
            for i in range(2):
                at = pl.ds(pl.multiple_of((place ^ t) * block + i * size, block), block)
                high[slot, at, :], low[slot, at, :] = split(part[i])


def forms_of(value):
    count = value.shape[0] // 2
    return split(both_forms(value[:count], value[count:]))


def apply_map(left, pair):
    (high, low), (right_high, right_low) = left, pair
    count = high.shape[0]
    dot = functools.partial(jnp.dot, preferred_element_type=F32)
    both = dot(jnp.concatenate([high, low], axis=0), right_high)
    return both[:count] + (both[count:] + dot(high, right_low))


def stacked(ref):
    return jnp.concatenate([ref[0], ref[1]], axis=0)


def put(ref, value, at=slice(None)):
    count = value.shape[0] // 2
    ref[0, :, at] = value[:count]
    ref[1, :, at] = value[count:]


def row_pairs(packs, slot):
    count = len(packs) // 2
    return [(packs[r][slot], packs[count + r][slot]) for r in range(count)]


def apply_maps(left, packs, slot):
    return jnp.concatenate([apply_map(left, pair) for pair in row_pairs(packs, slot)], axis=1)


def stage_kernel(hop, final, early, kept, got, *refs):
    count = (2 if early else 3) if hop else 0
    before, refs = refs[:count], refs[count:]
    packs, outs = (refs[:-2], refs[-2:]) if final else (refs[:-3], refs[-3:])
    turn = lax.axis_index("chain").astype(jnp.int32) >> 1 == hop

    @pl.when(turn)
    def _():
        odd = chain_half() == 1
        mine, theirs = stacked(kept), stacked(got)
        first = jnp.where(odd, theirs, mine)
        if hop:
            first = first + apply_maps(forms_of(stacked(before[0])), packs, 0)
        second = jnp.where(odd, mine, theirs) + apply_maps(forms_of(first), packs, 1)
        if not final:
            put(outs[0], second)
        put(outs[-2], jnp.where(odd, second, first))
        put(outs[-1], jnp.where(odd, first, second))

    if hop:

        @pl.when(jnp.logical_not(turn))
        def _():
            outs[-2][...] = before[1][...]
            if not early:
                outs[-1][...] = before[2][...]


def half_kernel(side, chunks, hops, *refs):
    parts, (out, block, sems) = refs[:-3 - side], refs[-3:]
    half = block.shape[2]
    first = pl.multiple_of(jnp.where(chain_half() == side, 0, half), half)
    last = lax.axis_index("chain").astype(jnp.int32) >> 1 == hops
    copies = []
    for i in range(2):
        pieces = [p[i] for p in parts]
        if len(pieces) > chunks:
            pieces = [jnp.where(last, pieces[1], pieces[0])] + pieces[2:]
        block[i] = jnp.concatenate(pieces, axis=0).T
        copies.append(pltpu.make_async_copy(block.at[i], out.at[i, :, pl.ds(first, half)], sems.at[i]))
        copies[i].start()
    for copy in copies:
        copy.wait()


def body(inverses, couplings, sources, counts):
    own_inverse, own_coupling, own_source = inverses[0], couplings[0], sources[0]
    orbitals, block = own_inverse.shape[1:]
    width = own_source.shape[2]
    half = width // 2
    spans = column_spans(half)
    pieces = lax.axis_size("col")
    far = pieces // 2
    chain_length = lax.axis_size("chain")
    active = (lax.broadcasted_iota(jnp.int32, (8, orbitals), 1) < counts[0]).astype(F32)
    rows = orbitals // ROW_CHUNKS
    flops = 8 * orbitals * orbitals

    couple = kernel_call(
        functools.partial(couple_kernel, pieces),
        [own_coupling],
        [((2 * block, 2 * orbitals), BF16)] * 2,
        flops,
    )
    source = kernel_call(
        functools.partial(source_kernel, pieces),
        [own_source],
        [((2, width, 2 * orbitals), BF16)] * 2,
        flops,
    )
    inverse, packs = [], []
    for r in range(ROW_CHUNKS):
        source_rows = lax.optimization_barrier(own_inverse) if r else own_inverse
        parts = gathered(source_rows[:, r * rows:(r + 1) * rows])
        inverse += parts
        (near,) = kernel_call(
            near_kernel, [*couple, *parts[:far]], [((2 * block, rows), F32)], flops * block
        )
        (own_map,) = kernel_call(
            functools.partial(map_kernel, r * rows),
            [active, *couple, near, *parts[far:]],
            [((2, block, rows), F32)],
            flops * block // ROW_CHUNKS,
        )
        same = gathered(own_map)
        other_map = exchange(own_map, "chain", 1)
        if r % 2 == 0:
            other = [other_map] + [None] * (pieces - 1)
            for t in range(1, far):
                other[t] = exchange(other_map, "col", t)
            for t in range(far, pieces):
                if t == far:
                    other[t] = exchange(same[t], "chain", 1)
                else:
                    other[t] = exchange(other[far], "col", t ^ far)
        else:
            other = gathered(other_map)
        packs.append(
            kernel_call(
                functools.partial(pack_kernel, pieces),
                    [*same, *other],
                [((2, 2 * orbitals, rows), BF16)] * 2,
                flops,
            )
        )
    packs = [p[0] for p in packs] + [p[1] for p in packs]
    shapes = [(2, end - start, orbitals) for start, end in spans]
    offsets = kernel_call(
        functools.partial(offset_kernel, ROW_CHUNKS, pieces, spans),
        [active, *source, *inverse],
        [(shape, F32) for shape in shapes] * 2,
        flops * width,
    )
    kept, sent = offsets[:CHUNKS], offsets[CHUNKS:]
    hops = chain_length // 2 - 1
    got = [exchange(sent[c], "chain", 1) for c in range(CHUNKS)]
    held = [[] for _ in range(CHUNKS)]
    keep, back = [], []
    for hop in range(hops + 1):
        final = hop == hops
        pairs = [(2 * hop + i, 2 * hop + 2 + i) for i in range(2)]
        for c in range(CHUNKS):
            *passed, mine, theirs = kernel_call(
                functools.partial(stage_kernel, hop, final, final and c == 0),
                    [kept[c], got[c], *held[c], *packs],
                [(shapes[c], F32)] * (2 if final else 3),
                flops * half,
            )
            if not final:
                if hop:
                    come = lax.ppermute(passed[0], "chain", pairs)
                else:
                    come = between(passed[0], {i: i ^ 2 for i in range(4)})
                held[c] = [come, mine, theirs]
                if c == 0 and hop == hops - 1:
                    early = between(held[c].pop(), {i: i ^ 1 for i in range(2 * hops)})
                continue
            keep.append(mine)
            if c == 0 and hops:
                own = [(2 * hops + i, 2 * hops + 1 - i) for i in range(2)]
                back += [early, lax.ppermute(theirs, "chain", own)]
            else:
                back.append(exchange(theirs, "chain", 1))
    out = None
    for side, parts in enumerate((keep, back)):
        out = pl.pallas_call(
            functools.partial(half_kernel, side, CHUNKS, hops),
            out_shape=jax.ShapeDtypeStruct((2, orbitals, width), F32),
            in_specs=[WHOLE] * len(parts) + [pl.BlockSpec(memory_space=pl.ANY)] * side,
            out_specs=pl.BlockSpec(memory_space=pl.ANY),
            scratch_shapes=[pltpu.VMEM((2, orbitals, half), F32), pltpu.SemaphoreType.DMA((2,))],
            input_output_aliases={len(parts): 0} if side else {},
            compiler_params=pltpu.CompilerParams(vmem_limit_bytes=24 * 2**20),
            cost_estimate=pl.CostEstimate(flops=flops, bytes_accessed=4096, transcendentals=0),
        )(*parts, *([out] if side else []))
    return out[None]


def solution(mesh):
    placed = (
        P("chain", None, None, "col"),
        P("chain", None, None, "col"),
        P("chain", None, None, "col"),
        P("chain"),
    )
    return jax.shard_map(
        body, mesh=mesh, in_specs=placed, out_specs=P("chain", None, None, "col"), check_vma=False
    )
```
